32 devices in a mesh: dp: 32 (over z, y, x, core), mp: 1.
Axes of the slice: x: 2, y: 2, z: 4, core: 2. Of those that a mesh axis runs over, the one named last changes fastest.
Arguments:
- gradients: bfloat16 [32, 512, 6144], P('dp', None, 'mp'), may hold values from -48 to 48
- weights: bfloat16 [512, 6144], P(None, 'mp'), may hold values from -3 to 3
- master: float32 [512, 6144], P('dp', 'mp'), may hold values from -6 to 6
- moment_one: float32 [512, 6144], P('dp', 'mp'), may hold values from -6 to 6
- moment_two: float32 [512, 6144], P('dp', 'mp'), may hold values from 0.25 to 4
- group_ids: int32 [512], replicated, may hold values from 0 to 15, never falling along the last dimension, each value on 1 to 64 neighbouring positions
Outputs:
- new_weights: bfloat16 [512, 6144], P(None, 'mp')
- new_master: float32 [512, 6144], P('dp', 'mp')
- new_first: float32 [512, 6144], P('dp', 'mp')
- new_second: float32 [512, 6144], P('dp', 'mp')
The draws below stay inside these ranges and needn't reach their ends.
Inputs may be any that keep to these rules, and one draw needn't show every extreme that they name: `group_ids`: group numbers never fall along the rows; each group has 1 to 64 rows and every group is present.
All inputs are finite; a program needn't handle non-finite values.
Results may differ from the reference program's by a relative error of at most 0.001.
The reference program's roundings to bfloat16 on the way count: a program that leaves them out, or rounds other values in their place, can miss the bound.
Values may be sent and summed in bfloat16 or wider, within the bound.
A program may use at most 64 MiB of HBM per device.

```python
import math
import jax
import jax.numpy as jnp
import numpy as np
from jax import lax

D = 6144
MOST = 64
ROWS_ALL = 512
GROUPS = 16
N_DP = 32


def raised(drawn, own_key, source, target, shards_of, factor):
    def block_of(dim):
        return (jnp.arange(drawn.shape[dim]) // (drawn.shape[dim] // shards_of)).reshape((-1,) + (1,) * (drawn.ndim - 1 - dim))

    first = jax.random.permutation(own_key, shards_of)[block_of(target)]
    other_side = (block_of(target) + shards_of // 2) % shards_of
    return jnp.where((block_of(source) == first) | (block_of(source) == other_side), factor * drawn, drawn)


def level_of(rng, extent, split, low, top_value):
    level = 1.0
    for axis_at, shards_of in split:
        draws = jax.random.uniform(jax.random.fold_in(jax.random.fold_in(rng, 6), axis_at), (shards_of,), jnp.float32, low / len(split), top_value / len(split))
        level = level * jnp.repeat(jnp.exp(draws), extent[axis_at] // shards_of).reshape((-1,) + (1,) * (len(extent) - 1 - axis_at))
    return level


def length_profile(amount, total, limit, slope):
    portions = [(1 << 20) // math.isqrt(grade ** slope) + 1 for grade in range(2, amount + 1)]
    rest, holding = total - limit - (amount - 1), [1] * (amount - 1)
    while rest > 0:
        candidates = [i for i in range(amount - 1) if holding[i] < limit]
        pool, budget = sum([portions[i] for i in candidates]), rest
        for i in candidates:
            more = min(limit - holding[i], max(1, budget * portions[i] // pool), rest)
            holding[i] = holding[i] + more
            rest = rest - more
    return np.array([limit] + holding)


def uneven(rng, number_of, total, most, lean):
    if number_of == 2:
        one = jax.random.randint(rng, (), max(1, total - most), min(most, total - 1) + 1)
        return jnp.stack([one, total - one])
    sizes = jnp.asarray(length_profile(number_of, total, most, lean), jnp.int32)
    pairs = (number_of - 1) // 2
    giver, sink = sizes[1:1 + 2 * pairs:2], sizes[2:2 + 2 * pairs:2]
    slack = jnp.minimum(giver - 1, most - sink)
    moved = jax.random.randint(jax.random.fold_in(rng, 1), (pairs,), 0, 1 << 20) % (slack + 1)
    sizes = sizes.at[1:1 + 2 * pairs:2].set(giver - moved).at[2:2 + 2 * pairs:2].set(sink + moved)
    return sizes[jax.random.permutation(jax.random.fold_in(rng, 2), number_of)]


def normal_values(stream_key, dims, deviation, most, shards=(), held_as=jnp.bfloat16):
    entries = deviation * jax.random.normal(stream_key, dims, jnp.float32)
    if shards:
        entries = entries * level_of(stream_key, dims, shards, -0.22, 0.18)
    return jnp.clip(entries, -most, most).astype(held_as)


def gaussian_with(stream_key, dims, scale, limit, pieces, heavy, kind=jnp.bfloat16):
    entries = scale * jax.random.normal(stream_key, dims, jnp.float32)
    if pieces:
        entries = entries * level_of(stream_key, dims, pieces, -0.22, 0.18)
    return jnp.clip(raised(entries, jax.random.fold_in(stream_key, 3), *heavy), -limit, limit).astype(kind)


def setup_inputs(seed: int = 0) -> dict:
    key_list = jax.random.split(jax.random.key(seed), 7)
    return {
        "gradients": gaussian_with(key_list[0], (N_DP, ROWS_ALL, D), 8.0, 48.0, ((0, 32),), (0, 1, 32, 2.75)),
        "weights": normal_values(key_list[1], (ROWS_ALL, D), 0.5, 3.0),
        "master": normal_values(key_list[2], (ROWS_ALL, D), 1.0, 6.0, ((0, 32),), jnp.float32),
        "moment_one": normal_values(key_list[3], (ROWS_ALL, D), 1.0, 6.0, ((0, 32),), jnp.float32),
        "moment_two": jnp.clip(jnp.exp(math.log(4.0) - 2.7725887 * jax.random.uniform(key_list[4], (ROWS_ALL, D), jnp.float32) ** level_of(key_list[4], (ROWS_ALL, D), ((0, 32),), -0.2, 0.2)), 0.25, 4.0),
        "group_ids": jnp.searchsorted(jnp.cumsum(uneven(key_list[5], GROUPS, ROWS_ALL, MOST, 0)), jnp.arange(ROWS_ALL), side="right").astype(jnp.int32),
    }


beta_one = 0.9
beta_two = 0.999
adam_eps = 1e-06
weight_decay = 0.01
learn_rate = 0.04
step_count = 100

def reference(gradients, weights, master, moment_one, moment_two, group_ids):
    grad_mean = lax.optimization_barrier(jnp.sum(gradients, axis=0, dtype=jnp.float32)) / N_DP
    new_first = beta_one * moment_one + (1.0 - beta_one) * grad_mean
    new_second = beta_two * moment_two + (1.0 - beta_two) * grad_mean * grad_mean
    correct_one = 1.0 - beta_one ** step_count
    correct_two = 1.0 - beta_two ** step_count
    update = new_first / correct_one / (jnp.sqrt(new_second / correct_two) + adam_eps) + weight_decay * master
    member = (group_ids[:, None] == jnp.arange(GROUPS, dtype=jnp.int32)[None, :]).astype(jnp.float32)
    weight_sq = jnp.dot(lax.optimization_barrier(jnp.sum(master * master, axis=1)), member, precision=lax.Precision.HIGHEST)
    update_sq = jnp.dot(lax.optimization_barrier(jnp.sum(update * update, axis=1)), member, precision=lax.Precision.HIGHEST)
    trust_ratio = jnp.sqrt(weight_sq / (update_sq + 1e-06))
    row_ratio = jnp.dot(member, trust_ratio, precision=lax.Precision.HIGHEST)
    step_size = learn_rate * row_ratio[:, None] * update
    new_master = master - step_size
    delta_bf = lax.optimization_barrier((-step_size).astype(jnp.bfloat16))
    new_weights = (weights.astype(jnp.float32) + delta_bf.astype(jnp.float32)).astype(jnp.bfloat16)
    return (new_weights, new_master, new_first, new_second)
```

```python
import functools

import jax
import jax.numpy as jnp
from jax import lax
from jax.experimental import pallas as pl
from jax.experimental.pallas import tpu as pltpu
from jax.sharding import PartitionSpec as P

beta_one = 0.9
beta_two = 0.999
adam_eps = 1e-06
weight_decay = 0.01
learn_rate = 0.04
step_count = 100

MESH = pl.DeviceIdType.MESH
F32, BF16, I16, I32 = jnp.float32, jnp.bfloat16, jnp.int16, jnp.int32
WIDTH = 512
LANES = 128
UNROLL = 4
TOP = 32700.0
TINY = 1e-30


def flipped(bit, flag):
    return bit + flag - 2 * bit * flag


def kernel_orders(n, chunks):
    orders = []
    for k in range(chunks):
        order = list(range(n))
        if n > 3:
            order[1:4] = [2, 3, 1] if k % 2 else [1, 3, 2]
        orders.append(order)
    return orders


def schedule(n, chunks):
    tasks = []
    for k in range(chunks):
        u = k // 2
        for s in range(n):
            tasks.append((u + 1.0 * s, -s, k, "R"))
        for s in range(n):
            tasks.append((u + 1.0 * (n + s), -(n + s), k, "A"))
    tasks.sort()
    out = []
    for _, s, k, what in tasks:
        s = -s
        out.append((what, k, s if what == "R" else s - n))
    return out


def kernel(
    n, mp, width, levels_n, ids_ref, grad_ref, w_ref, master_hbm, m1_hbm, m2_hbm,
    out_ref, new_master_ref, new_first_ref, new_second_ref,
    mine, raw, temp, kept, codes_out, codes_in, scales_out, scales_in, held, held_scale,
    update, sums, member, ratio, tiles, master_ref, m1_ref, m2_ref,
    mine_sem, w_sem, own_sem, raw_send, raw_recv, rs_send, rs_recv, rs_send2, rs_recv2,
    ag_send, ag_recv, ag_send2, ag_recv2, t_send, t_recv,
):
    me = lax.axis_index("dp")
    bits = [(me // 2**i) % 2 for i in range(n)]
    replicas = 2**n
    rows, cols = master_ref.shape
    chunks = cols // width
    lane_groups = width // LANES
    orders = kernel_orders(n, chunks)

    def span(k):
        return pl.ds(k * width, width)

    def partner(flips):
        return sum(2**i * (1 - bits[i] if flips >> i & 1 else bits[i]) for i in range(n))

    low = min(n, 3)
    levels = [[{"dp": partner(f)} for f in range(1, 2**low)]]
    if n > low:
        levels.append([{"dp": partner(f << low)} for f in range(1, 2 ** (n - low))])
    if mp > 1:
        mine_mp = lax.axis_index("mp")
        places = mp.bit_length() - 1
        mp_bits = [(mine_mp // 2**i) % 2 for i in range(places)]
        levels.append([
            {"mp": sum(2**i * (1 - mp_bits[i] if f >> i & 1 else mp_bits[i]) for i in range(places))}
            for f in range(1, mp)
        ])

    w_copy = pltpu.make_async_copy(w_ref, out_ref, w_sem)
    own_copies = [
        pltpu.make_async_copy(src, dst, own_sem.at[i])
        for i, (src, dst) in enumerate([(master_hbm, master_ref), (m1_hbm, m1_ref), (m2_hbm, m2_ref)])
    ]
    mine_copies = [
        pltpu.make_async_copy(grad_ref.at[:, bits[0], :, span(k)], mine.at[k], mine_sem.at[k])
        for k in range(chunks)
    ]
    for copy in mine_copies:
        copy.start()

    barrier = pltpu.get_barrier_semaphore()
    greeted = [target for level in levels for target in level]
    for target in greeted:
        pl.semaphore_signal(barrier, inc=1, device_id=target, device_id_type=MESH)
    pl.semaphore_wait(barrier, len(greeted))

    started = []

    def send(src, dst, send_sem, recv_sem, target):
        copy = pltpu.make_async_remote_copy(
            src_ref=src, dst_ref=dst, send_sem=send_sem, recv_sem=recv_sem,
            device_id=target, device_id_type=MESH,
        )
        copy.start()
        started.append(copy)
        return copy

    rs = {}
    for k in range(chunks):
        rs[k, 0] = [send(
            grad_ref.at[:, 1 - bits[0], :, span(k)], raw.at[k],
            raw_send.at[k], raw_recv.at[k], {"dp": partner(1)},
        )]
    for copy in own_copies:
        copy.start()
    w_copy.start()

    lane = lax.broadcasted_iota(I32, (1, LANES), 1)

    @pl.loop(0, replicas * rows, unroll=8)
    def _(r):
        member[pl.ds(r, 1), :] = jnp.where(lane == ids_ref[r], 1.0, 0.0).astype(F32)

    sums[...] = jnp.zeros_like(sums)
    correct_one = 1.0 - beta_one**step_count
    correct_two = 1.0 - beta_two**step_count

    def lanes_of(g):
        return pl.ds(g * LANES, LANES)

    def largest(values, so_far):
        for g in range(lane_groups):
            part = jnp.abs(values[:, g * LANES:(g + 1) * LANES])
            for h in range(rows // 8):
                so_far = jnp.maximum(so_far, part[h * 8:(h + 1) * 8])
        return so_far

    def scale_of(most):
        top = jnp.maximum(jnp.max(most, axis=0, keepdims=True), TINY)
        return top * (1.0 / TOP), TOP / top

    def code(value):
        return jnp.round(value).astype(I32).astype(I16)

    def wide(row):
        return jnp.concatenate([row] * lane_groups, axis=1)

    def rest_of(order, d):
        rest = 0
        for i in range(n - 1):
            b = order[n - 1 - i]
            rest = rest + 2 ** (b - 1) * flipped(bits[b], (d // 2**i) % 2)
        return rest

    def reduce(k, s):
        order = orders[k]
        for copy in rs[k, s]:
            copy.wait_recv()
        if s == 0:
            mine_copies[k].wait()

        if s:
            scale_in = wide(scales_in[s - 1][k])

        def total(d):
            if s == 0:
                rest = rest_of(order, d)
                return mine[k, rest].astype(F32) + raw[k, rest].astype(F32)
            got = codes_in[s - 1][k, d].astype(F32) * scale_in
            if s == 1:
                rest = rest_of(order, d)
                return mine[k, rest].astype(F32) + raw[k, rest].astype(F32) + got
            return kept[k, d] + got

        if s < n - 1:
            half = 2 ** (n - 2 - s)

            @pl.loop(0, half, init_carry=jnp.zeros((8, LANES), F32), unroll=min(UNROLL, half))
            def most(d, so_far):
                value = total(half + d)
                temp[d] = value
                return largest(value, so_far)

            scale, inverse = scale_of(most)
            scales_out[s][k] = scale
            spread = wide(inverse)

            @pl.loop(0, half, unroll=min(UNROLL, half))
            def _(d):
                codes_out[s][k, d] = code(temp[d] * spread)

            target = {"dp": partner(1 << order[s + 1])}
            rs[k, s + 1] = [
                send(codes_out[s].at[k], codes_in[s].at[k], rs_send.at[k, s], rs_recv.at[k, s], target),
                send(scales_out[s].at[k], scales_in[s].at[k], rs_send2.at[k, s], rs_recv2.at[k, s], target),
            ]
            if s:

                @pl.loop(0, half, unroll=min(UNROLL, half))
                def _(d):
                    kept[k, d] = total(d)
            return
        if k == first_done:
            for copy in own_copies:
                copy.wait()
        grad_mean = total(0) / replicas
        master = master_ref[:, span(k)]
        new_first = beta_one * m1_ref[:, span(k)] + (1.0 - beta_one) * grad_mean
        new_second = beta_two * m2_ref[:, span(k)] + (1.0 - beta_two) * grad_mean * grad_mean
        change = (
            new_first / correct_one / (jnp.sqrt(new_second / correct_two) + adam_eps)
            + weight_decay * master
        )
        scale, inverse = scale_of(largest(change, jnp.zeros((8, LANES), F32)))
        held_scale[k, 0] = scale
        held[k, 0] = code(change * wide(inverse))
        gather(k, 0)
        update[:, span(k)] = change
        new_first_ref[:, span(k)] = new_first
        new_second_ref[:, span(k)] = new_second
        for i, value in enumerate((master, change)):
            square = value * value
            sums[i] += sum(square[:, g * LANES:(g + 1) * LANES] for g in range(lane_groups))

    ag = {}

    def gather(k, s):
        target = {"dp": partner(1 << orders[k][n - 1 - s])}
        here, there = pl.ds(0, 2**s), pl.ds(2**s, 2**s)
        ag[k, s] = [
            send(held.at[k, here], held.at[k, there], ag_send.at[k, s], ag_recv.at[k, s], target),
            send(held_scale.at[k, here], held_scale.at[k, there], ag_send2.at[k, s], ag_recv2.at[k, s], target),
        ]

    def expand(k, s):
        for copy in ag[k, s]:
            copy.wait_recv()
        if s < n - 1:
            gather(k, s + 1)

    trust_state = {}
    trust_at = [0]

    def trust_send(level):
        slots = tiles[level]
        slots[0] = trust_state["sums"]
        copies = []
        for f, target in enumerate(levels[level], 1):
            at = trust_at[0]
            copies.append(send(slots.at[0], slots.at[f], t_send.at[at], t_recv.at[at], target))
            trust_at[0] += 1
        trust_state["copies"] = copies

    def trust_start():
        own = member[pl.ds(pl.multiple_of(me * rows, rows), rows), :]
        w_part = jnp.sum(own * jnp.sum(sums[0], axis=1, keepdims=True), axis=0, keepdims=True)
        u_part = jnp.sum(own * jnp.sum(sums[1], axis=1, keepdims=True), axis=0, keepdims=True)
        sub = lax.broadcasted_iota(I32, (8, LANES), 0)
        trust_state["sums"] = jnp.where(sub == 0, w_part, u_part)
        trust_send(0)

    def trust_next(level):
        total = trust_state["sums"]
        for f, copy in enumerate(trust_state["copies"], 1):
            copy.wait_recv()
            total = total + tiles[level][f]
        trust_state["sums"] = total
        if level + 1 < len(levels):
            trust_send(level + 1)
            return
        trust = jnp.sqrt(total[0:1] / (total[1:2] + 1e-06))

        @pl.loop(0, replicas, unroll=4)
        def _(d):
            at = pl.ds(pl.multiple_of(d * rows, rows), rows)
            row_ratio = jnp.sum(member[at, :] * trust, axis=1, keepdims=True)
            ratio[at, :] = jnp.broadcast_to(-learn_rate * row_ratio, (rows, LANES))

    def own_master():
        at = pl.ds(pl.multiple_of(me * rows, rows), rows)
        down = ratio[at, :]
        for g in range(cols // LANES):
            new_master_ref[:, lanes_of(g)] = master_ref[:, lanes_of(g)] + down * update[:, lanes_of(g)]

    def apply(k):
        @pl.loop(0, replicas, unroll=min(UNROLL, replicas))
        def _(d):
            owner = 0
            for i in range(n):
                b = orders[k][n - 1 - i]
                owner = owner + 2**b * flipped(bits[b], (d // 2**i) % 2)
            at = pl.ds(pl.multiple_of(owner * rows, rows), rows)
            factor = ratio[at, :] * held_scale[k, d]
            delta = (held[k, d].astype(F32) * wide(factor)).astype(BF16)
            out_ref[owner, :, span(k)] = (
                out_ref[owner, :, span(k)].astype(F32) + delta.astype(F32)
            ).astype(BF16)

    order = schedule(n, chunks)
    ends = [i for i, task in enumerate(order) if task[0] == "R" and task[2] == n - 1]
    first_done = order[ends[0]][1]
    last_update = ends[-1]
    applied, gathered, trusted, since = set(), [], -1, 0
    for i, (what, k, s) in enumerate(order):
        if what == "R":
            reduce(k, s)
        else:
            expand(k, s)
            if s == n - 1:
                gathered.append(k)
        if i == last_update:
            trust_start()
            trusted, since = 0, 0
        elif 0 <= trusted < len(levels):
            since += 1
            if since == 2:
                trust_next(trusted)
                trusted, since = trusted + 1, 0
                if trusted == len(levels):
                    own_master()
                    w_copy.wait()
        elif trusted == len(levels):
            for j in [j for j in gathered if j not in applied][:2]:
                apply(j)
                applied.add(j)
    while trusted < len(levels):
        trust_next(trusted)
        trusted += 1
        if trusted == len(levels):
            own_master()
            w_copy.wait()
    for j in gathered:
        if j not in applied:
            apply(j)
    for copy in started:
        copy.wait_send()


def solution(mesh):
    replicas, mp = mesh.shape["dp"], mesh.shape["mp"]
    n = replicas.bit_length() - 1

    def on_device(gradients, weights, master, moment_one, moment_two, group_ids):
        rows_all, cols = weights.shape
        rows = master.shape[0]
        width = WIDTH if cols % WIDTH == 0 else LANES
        chunks = cols // width
        low = min(n, 3)
        counts = [2**low] + ([2 ** (n - low)] if n > low else []) + ([mp] if mp > 1 else [])
        anywhere = pl.BlockSpec(memory_space=pl.ANY)
        vmem = pl.BlockSpec(memory_space=pltpu.VMEM)
        own = pltpu.VMEM((rows, cols), F32)
        dma = pltpu.SemaphoreType.DMA
        tiles_n = sum(c - 1 for c in counts)
        halves = [2 ** (n - 2 - s) for s in range(n - 1)]
        codes = [pltpu.VMEM((chunks, half, rows, width), I16) for half in halves]
        scales = [pltpu.VMEM((chunks, 1, LANES), F32) for _ in halves]
        new_weights, new_master, new_first, new_second = pl.pallas_call(
            functools.partial(kernel, n, mp, width, len(counts)),
            out_shape=(pltpu.VMEM((replicas, rows, cols), BF16), own, own, own),
            in_specs=[pl.BlockSpec(memory_space=pltpu.SMEM)] + [anywhere] * 5,
            out_specs=(vmem, vmem, vmem, vmem),
            scratch_shapes=[
                pltpu.VMEM((chunks, replicas // 2, rows, width), BF16),
                pltpu.VMEM((chunks, replicas // 2, rows, width), BF16),
                pltpu.VMEM((replicas // 4, rows, width), F32),
                pltpu.VMEM((chunks, max(replicas // 8, 1), rows, width), F32),
                codes, codes, scales, scales,
                pltpu.VMEM((chunks, replicas, rows, width), I16),
                pltpu.VMEM((chunks, replicas, 1, LANES), F32),
                pltpu.VMEM((rows, cols), F32),
                pltpu.VMEM((2, rows, LANES), F32),
                pltpu.VMEM((rows_all, LANES), F32),
                pltpu.VMEM((rows_all, LANES), F32),
                [pltpu.VMEM((c, 8, LANES), F32) for c in counts],
                own, own, own,
                dma((chunks,)), dma, dma((3,)),
                dma((chunks,)), dma((chunks,)),
                dma((chunks, n - 1)), dma((chunks, n - 1)), dma((chunks, n - 1)), dma((chunks, n - 1)),
                dma((chunks, n)), dma((chunks, n)), dma((chunks, n)), dma((chunks, n)),
                dma((tiles_n,)), dma((tiles_n,)),
            ],
            compiler_params=pltpu.CompilerParams(
                collective_id=0, has_side_effects=True, vmem_limit_bytes=52 * 2**20
            ),
        )(
            group_ids,
            gradients.reshape(replicas // 2, 2, rows, cols),
            weights.reshape(replicas, rows, cols),
            master, moment_one, moment_two,
        )
        return new_weights.reshape(rows_all, cols), new_master, new_first, new_second

    return jax.shard_map(
        on_device,
        mesh=mesh,
        in_specs=(P("dp", None, "mp"), P(None, "mp"), P("dp", "mp"), P("dp", "mp"), P("dp", "mp"), P()),
        out_specs=(P(None, "mp"), P("dp", "mp"), P("dp", "mp"), P("dp", "mp")),
        check_vma=False,
    )
```

```python
import functools

import jax
import jax.numpy as jnp
from jax import lax
from jax.experimental import pallas as pl
from jax.experimental.pallas import tpu as pltpu
from jax.sharding import PartitionSpec as P

beta_one = 0.9
beta_two = 0.999
adam_eps = 1e-06
weight_decay = 0.01
learn_rate = 0.04
step_count = 100

MESH = pl.DeviceIdType.MESH
F32, BF16, I16, I32 = jnp.float32, jnp.bfloat16, jnp.int16, jnp.int32
WIDTH = 512
LANES = 128
STATIC = 8
SKEW = 2
TOP = 32700.0
TINY = 1e-30


def flipped(bit, flag):
    if isinstance(flag, int):
        return 1 - bit if flag else bit
    return bit + flag - 2 * bit * flag


def over_slots(first, count, step):
    fixed = min(count, STATIC)
    places = count.bit_length() - 1
    low = fixed.bit_length() - 1

    def run(high):
        if len(high) < places - low:

            @pl.loop(0, 2)
            def _(bit):
                run([bit] + high)
            return
        for i in range(fixed):
            step([i >> p & 1 for p in range(low)] + high + ([1] if first else []))

    run([])


def slot(flags):
    return sum(2**p * flag for p, flag in enumerate(flags))


def kernel_orders(n, chunks):
    orders = []
    for k in range(chunks):
        order = list(range(n))
        if n > 3:
            order[1:4] = [2, 3, 1] if k % 2 else [1, 3, 2]
        orders.append(order)
    return orders


def schedule(n, chunks, levels):
    tasks = []
    for k in range(chunks):
        u = k // 2
        for s in range(2 * n):
            what = ("R", k, s) if s < n else ("A", k, s - n)
            tasks.append((u + SKEW * s, 2 * n - s, k, what))
    tasks.sort()
    order = [what for *_, what in tasks]
    last = max(i for i, task in enumerate(order) if task[0] == "R")
    out, ready, level, since = [], [], 0, 0
    for i, task in enumerate(order):
        out.append(task)
        if task[0] == "A" and task[2] == n - 1:
            ready.append(task[1])
        if i == last:
            out.append(("T", 0, 0))
            level, since = 1, 0
        elif 0 < level <= levels:
            since += 1
            if since == 2:
                out.append(("T", 0, level))
                level, since = level + 1, 0
        elif level > levels:
            for k in ready[:2]:
                out.append(("P", k, 0))
            ready = ready[2:]
    while level <= levels:
        out.append(("T", 0, level))
        level += 1
    return out + [("P", k, 0) for k in ready]


def kernel(
    n, mp, width, levels_n, ids_ref, grad_ref, w_ref, master_hbm, m1_hbm, m2_hbm,
    out_ref, new_master_ref, new_first_ref, new_second_ref,
    mine, raw, temp, peak, kept, codes_out, codes_in, scales_out, scales_in, held, held_scale,
    update, sums, member, ratio, tiles, state, units,
    mine_sem, w_sem, own_sem, raw_send, raw_recv, rs_send, rs_recv, ag_send, ag_recv, t_send, t_recv,
):
    me = lax.axis_index("dp")
    bits = [(me // 2**i) % 2 for i in range(n)]
    replicas = 2**n
    _, rows, cols = state.shape
    master_ref, m1_ref, m2_ref = (state.at[i] for i in range(3))
    chunks = cols // width
    lane_groups = width // LANES
    orders = kernel_orders(n, chunks)

    def span(k):
        return pl.ds(k * width, width)

    def partner(flips):
        return sum(2**i * (1 - bits[i] if flips >> i & 1 else bits[i]) for i in range(n))

    low = min(n, 3)
    levels = [[{"dp": partner(f)} for f in range(1, 2**low)]]
    if n > low:
        levels.append([{"dp": partner(f << low)} for f in range(1, 2 ** (n - low))])
    if mp > 1:
        mine_mp = lax.axis_index("mp")
        places = mp.bit_length() - 1
        mp_bits = [(mine_mp // 2**i) % 2 for i in range(places)]
        levels.append([
            {"mp": sum(2**i * (1 - mp_bits[i] if f >> i & 1 else mp_bits[i]) for i in range(places))}
            for f in range(1, mp)
        ])

    w_copy = pltpu.make_async_copy(w_ref, out_ref, w_sem)
    own_copies = [
        pltpu.make_async_copy(src, state.at[i], own_sem) for i, src in enumerate([master_hbm, m1_hbm, m2_hbm])
    ]
    mine_copies = [
        pltpu.make_async_copy(grad_ref.at[:, bits[0], :, span(k)], mine.at[k], mine_sem)
        for k in range(chunks)
    ]
    for copy in mine_copies:
        copy.start()

    barrier = pltpu.get_barrier_semaphore()
    greeted = [target for level in levels for target in level]
    for target in greeted:
        pl.semaphore_signal(barrier, inc=1, device_id=target, device_id_type=MESH)
    pl.semaphore_wait(barrier, len(greeted))

    def finish(ref, sem):
        pltpu.make_async_copy(ref, ref, sem).wait()

    def finish_coded(slots, scales, sem):
        row = LANES * 4
        count = (slots * rows * width * 2 + scales * row) // row
        finish(units.at[pl.ds(0, count)], sem)

    def send(src, dst, send_sem, recv_sem, target):
        copy = pltpu.make_async_remote_copy(
            src_ref=src, dst_ref=dst, send_sem=send_sem, recv_sem=recv_sem,
            device_id=target, device_id_type=MESH,
        )
        copy.start()

    for k in range(chunks):
        send(
            grad_ref.at[:, 1 - bits[0], :, span(k)], raw.at[k], raw_send, raw_recv.at[k], {"dp": partner(1)}
        )
    for copy in own_copies:
        copy.start()
    w_copy.start()

    lane = lax.broadcasted_iota(I32, (1, LANES), 1)

    @pl.loop(0, replicas * rows, unroll=8)
    def _(r):
        member[pl.ds(r, 1), :] = jnp.where(lane == ids_ref[r], 1.0, 0.0).astype(F32)

    sums[...] = jnp.zeros_like(sums)
    correct_one = 1.0 - beta_one**step_count
    correct_two = 1.0 - beta_two**step_count

    def lanes_of(g):
        return pl.ds(g * LANES, LANES)

    def largest(values, so_far):
        for g in range(lane_groups):
            part = jnp.abs(values[:, g * LANES:(g + 1) * LANES])
            for h in range(rows // 8):
                so_far = jnp.maximum(so_far, part[h * 8:(h + 1) * 8])
        return so_far

    def scale_of(most):
        top = jnp.maximum(jnp.max(most, axis=0, keepdims=True), TINY)
        return top * (1.0 / TOP), TOP / top

    def code(value):
        return jnp.round(value).astype(I32).astype(I16)

    def wide(row):
        return jnp.concatenate([row] * lane_groups, axis=1)

    def label_of(order, flags):
        label = [None] * n
        for i, flag in enumerate(flags):
            label[order[n - 1 - i]] = flipped(bits[order[n - 1 - i]], flag)
        for b in range(n):
            if label[b] is None:
                label[b] = bits[b]
        return label

    def both(k, flags):
        rest = sum(2 ** (b - 1) * bit for b, bit in enumerate(label_of(orders[k], flags)) if b)
        return mine[k, rest].astype(F32) + raw[k, rest].astype(F32)

    def reduce(k, s):
        order = orders[k]
        if s == 0:
            if k == first_taken:
                finish(mine, mine_sem)
            finish(raw.at[k], raw_recv.at[k])
        else:
            finish_coded(2 ** (n - 1 - s), 1, rs_recv.at[k, s - 1])
            scale_in = wide(scales_in[s - 1][k])

        def total(flags):
            if s == 0:
                return both(k, flags)
            d = slot(flags)
            got = codes_in[s - 1][k, d].astype(F32) * scale_in
            return (both(k, flags) if s == 1 else kept[k, d]) + got

        if s < n - 1:
            half = 2 ** (n - 2 - s)
            peak[...] = jnp.zeros_like(peak)

            def add(flags):
                value = total(flags)
                temp[slot(flags[:-1])] = value
                peak[...] = largest(value, peak[...])

            over_slots(half, half, add)
            scale, inverse = scale_of(peak[...])
            scales_out[s][k] = scale
            spread = wide(inverse)

            def encode(flags):
                d = slot(flags)
                codes_out[s][k, d] = code(temp[d] * spread)

            over_slots(0, half, encode)
            target = {"dp": partner(1 << order[s + 1])}
            send(codes_out[s].at[k], codes_in[s].at[k], rs_send.at[s, 0], rs_recv.at[k, s], target)
            send(scales_out[s].at[k], scales_in[s].at[k], rs_send.at[s, 1], rs_recv.at[k, s], target)
            if s:

                def keep(flags):
                    kept[k, slot(flags)] = total(flags)

                over_slots(0, half, keep)
            return
        if k == first_done:
            finish(state, own_sem)
        grad_mean = total([]) / replicas
        master = master_ref[:, span(k)]
        new_first = beta_one * m1_ref[:, span(k)] + (1.0 - beta_one) * grad_mean
        new_second = beta_two * m2_ref[:, span(k)] + (1.0 - beta_two) * grad_mean * grad_mean
        change = (
            new_first / correct_one / (jnp.sqrt(new_second / correct_two) + adam_eps)
            + weight_decay * master
        )
        scale, inverse = scale_of(largest(change, jnp.zeros((8, LANES), F32)))
        held_scale[k, 0] = scale
        held[k, 0] = code(change * wide(inverse))
        pass_on(k, -1)
        update[:, span(k)] = change
        new_first_ref[:, span(k)] = new_first
        new_second_ref[:, span(k)] = new_second
        for i, value in enumerate((master, change)):
            square = value * value
            sums[i] += sum(square[:, g * LANES:(g + 1) * LANES] for g in range(lane_groups))

    def gather(k, s, piece):
        target = {"dp": partner(1 << orders[k][n - 1 - s])}
        count = max(2 ** (s - 1), 1)
        first = count if s and piece else 0
        here, there = pl.ds(first, count), pl.ds(first + 2**s, count)
        send(held.at[k, here], held.at[k, there], ag_send.at[s, 0], ag_recv.at[k, s], target)
        send(held_scale.at[k, here], held_scale.at[k, there], ag_send.at[s, 1], ag_recv.at[k, s], target)

    def pass_on(k, s):
        if s + 1 < n:
            gather(k, s + 1, 1)
        if s + 2 < n:
            gather(k, s + 2, 0)

    def expand(k, s):
        finish_coded(2**s, 2**s, ag_recv.at[k, s])
        pass_on(k, s)

    trust_state = {}

    def trust_send(level):
        slots = tiles[level]
        slots[0] = trust_state["sums"]
        for f, target in enumerate(levels[level], 1):
            send(slots.at[0], slots.at[f], t_send.at[level], t_recv.at[level], target)

    def trust_start():
        own = member[pl.ds(pl.multiple_of(me * rows, rows), rows), :]
        w_part = jnp.sum(own * jnp.sum(sums[0], axis=1, keepdims=True), axis=0, keepdims=True)
        u_part = jnp.sum(own * jnp.sum(sums[1], axis=1, keepdims=True), axis=0, keepdims=True)
        sub = lax.broadcasted_iota(I32, (8, LANES), 0)
        trust_state["sums"] = jnp.where(sub == 0, w_part, u_part)
        trust_send(0)

    def trust_next(level):
        total = trust_state["sums"]
        others = len(levels[level])
        finish(tiles[level].at[pl.ds(1, others)], t_recv.at[level])
        for f in range(1, others + 1):
            total = total + tiles[level][f]
        trust_state["sums"] = total
        if level + 1 < len(levels):
            trust_send(level + 1)
            return
        trust = jnp.sqrt(total[0:1] / (total[1:2] + 1e-06))

        @pl.loop(0, replicas, unroll=4)
        def _(d):
            at = pl.ds(pl.multiple_of(d * rows, rows), rows)
            row_ratio = jnp.sum(member[at, :] * trust, axis=1, keepdims=True)
            ratio[at, :] = jnp.broadcast_to(-learn_rate * row_ratio, (rows, LANES))

    def own_master():
        at = pl.ds(pl.multiple_of(me * rows, rows), rows)
        down = ratio[at, :]
        for g in range(cols // LANES):
            new_master_ref[:, lanes_of(g)] = master_ref[:, lanes_of(g)] + down * update[:, lanes_of(g)]

    def apply(k):
        def one(flags):
            d = slot(flags)
            owner = sum(2**b * bit for b, bit in enumerate(label_of(orders[k], flags)))
            at = pl.ds(pl.multiple_of(owner * rows, rows), rows)
            factor = ratio[at, :] * held_scale[k, d]
            delta = (held[k, d].astype(F32) * wide(factor)).astype(BF16)
            out_ref[owner, :, span(k)] = (
                out_ref[owner, :, span(k)].astype(F32) + delta.astype(F32)
            ).astype(BF16)

        over_slots(0, replicas, one)

    order = schedule(n, chunks, len(levels))
    first_taken = order[0][1]
    first_done = next(k for what, k, s in order if what == "R" and s == n - 1)
    for what, k, s in order:
        if what == "R":
            reduce(k, s)
        elif what == "A":
            expand(k, s)
        elif what == "P":
            apply(k)
        elif s == 0:
            trust_start()
        else:
            trust_next(s - 1)
            if s == len(levels):
                own_master()
                w_copy.wait()
    finish(raw, raw_send)
    for s in range(n - 1):
        finish(codes_out[s], rs_send.at[s, 0])
        finish(scales_out[s], rs_send.at[s, 1])
    for s in range(n):
        finish(held.at[:, pl.ds(0, 2**s)], ag_send.at[s, 0])
        finish(held_scale.at[:, pl.ds(0, 2**s)], ag_send.at[s, 1])
    for i, slots in enumerate(tiles):
        finish(slots.at[pl.ds(1, len(levels[i]))], t_send.at[i])


def solution(mesh):
    replicas, mp = mesh.shape["dp"], mesh.shape["mp"]
    n = replicas.bit_length() - 1

    def on_device(gradients, weights, master, moment_one, moment_two, group_ids):
        rows_all, cols = weights.shape
        rows = master.shape[0]
        width = WIDTH if cols % WIDTH == 0 else LANES
        chunks = cols // width
        low = min(n, 3)
        counts = [2**low] + ([2 ** (n - low)] if n > low else []) + ([mp] if mp > 1 else [])
        anywhere = pl.BlockSpec(memory_space=pl.ANY)
        vmem = pl.BlockSpec(memory_space=pltpu.VMEM)
        own = pltpu.VMEM((rows, cols), F32)
        dma = pltpu.SemaphoreType.DMA
        halves = [2 ** (n - 2 - s) for s in range(n - 1)]
        codes = [pltpu.VMEM((chunks, half, rows, width), I16) for half in halves]
        scales = [pltpu.VMEM((chunks, 1, LANES), F32) for _ in halves]
        new_weights, new_master, new_first, new_second = pl.pallas_call(
            functools.partial(kernel, n, mp, width, len(counts)),
            out_shape=(pltpu.VMEM((replicas, rows, cols), BF16), own, own, own),
            in_specs=[pl.BlockSpec(memory_space=pltpu.SMEM)] + [anywhere] * 5,
            out_specs=(vmem, vmem, vmem, vmem),
            scratch_shapes=[
                pltpu.VMEM((chunks, replicas // 2, rows, width), BF16),
                pltpu.VMEM((chunks, replicas // 2, rows, width), BF16),
                pltpu.VMEM((replicas // 4, rows, width), F32),
                pltpu.VMEM((8, LANES), F32),
                pltpu.VMEM((chunks, max(replicas // 8, 1), rows, width), F32),
                codes, codes, scales, scales,
                pltpu.VMEM((chunks, replicas, rows, width), I16),
                pltpu.VMEM((chunks, replicas, 1, LANES), F32),
                pltpu.VMEM((rows, cols), F32),
                pltpu.VMEM((2, rows, LANES), F32),
                pltpu.VMEM((rows_all, LANES), F32),
                pltpu.VMEM((rows_all, LANES), F32),
                [pltpu.VMEM((c, 8, LANES), F32) for c in counts],
                pltpu.VMEM((3, rows, cols), F32),
                pltpu.VMEM((replicas // 2 * (rows * width // (2 * LANES) + 1), 1, LANES), F32),
                dma, dma, dma,
                dma, dma((chunks,)),
                dma((n - 1, 2)), dma((chunks, n - 1)),
                dma((n, 2)), dma((chunks, n)),
                dma((len(counts),)), dma((len(counts),)),
            ],
            compiler_params=pltpu.CompilerParams(
                collective_id=0, has_side_effects=True, vmem_limit_bytes=52 * 2**20
            ),
        )(
            group_ids,
            gradients.reshape(replicas // 2, 2, rows, cols),
            weights.reshape(replicas, rows, cols),
            master, moment_one, moment_two,
        )
        return new_weights.reshape(rows_all, cols), new_master, new_first, new_second

    return jax.shard_map(
        on_device,
        mesh=mesh,
        in_specs=(P("dp", None, "mp"), P(None, "mp"), P("dp", "mp"), P("dp", "mp"), P("dp", "mp"), P()),
        out_specs=(P(None, "mp"), P("dp", "mp"), P("dp", "mp"), P("dp", "mp")),
        check_vma=False,
    )
```

```python
import functools

import jax
import jax.numpy as jnp
from jax import lax
from jax.experimental import pallas as pl
from jax.experimental.pallas import tpu as pltpu
from jax.sharding import PartitionSpec as P

beta_one = 0.9
beta_two = 0.999
adam_eps = 1e-06
weight_decay = 0.01
learn_rate = 0.04
step_count = 100

MESH = pl.DeviceIdType.MESH
F32, BF16, I16, I32 = jnp.float32, jnp.bfloat16, jnp.int16, jnp.int32
WIDTH = 512
LANES = 128
STATIC = 8
STAGE_DUE = [0.00, 3.47, 6.19, 9.36, 13.72, 17.22, 21.30, 25.04, 29.23, 40.00]
STAGE_PACE = [2.37, 2.55, 2.91, 2.81, 2.56, 2.76, 2.48, 2.69, 4.82, 4.12]
TRUST_DUE = [26.48, 30.77, 35.67]
PUT_DUE = (33.46, 0.22)
TOP = 32700.0
TINY = 1e-30


def flipped(bit, flag):
    if isinstance(flag, int):
        return 1 - bit if flag else bit
    return bit + flag - 2 * bit * flag


def over_slots(first, count, step):
    fixed = min(count, STATIC)
    places = count.bit_length() - 1
    low = fixed.bit_length() - 1

    def run(high):
        if len(high) < places - low:

            @pl.loop(0, 2)
            def _(bit):
                run([bit] + high)
            return
        for i in range(fixed):
            step([i >> p & 1 for p in range(low)] + high + ([1] if first else []))

    run([])


def slot(flags):
    return sum(2**p * flag for p, flag in enumerate(flags))


def kernel_orders(n, chunks):
    orders = []
    for k in range(chunks):
        order = list(range(n))
        if n > 3:
            order[1:4] = [2, 3, 1] if k % 2 else [1, 3, 2]
        orders.append(order)
    return orders


def schedule(n, chunks, levels):
    if len(STAGE_DUE) == 2 * n:
        due, pace, trust, put = STAGE_DUE, STAGE_PACE, TRUST_DUE, PUT_DUE
    else:
        due, pace = [2.0 * s for s in range(2 * n)], [1.0] * (2 * n)
        trust, put = [due[-1]] * (levels + 1), (due[-1], 1.0)
    after, when = {}, {}
    for k in range(chunks):
        for s in range(2 * n):
            task = ("R", k, s) if s < n else ("A", k, s - n)
            after[task] = [last] if s else []
            when[task] = (due[s] + pace[s] * (k // 2), k)
            last = task
        after["P", k, 0] = [last, ("T", 0, levels)]
        when["P", k, 0] = (put[0] + put[1] * (k // 2), k)
    for level in range(levels + 1):
        after["T", 0, level] = [("T", 0, level - 1)] if level else [("R", k, n - 1) for k in range(chunks)]
        when["T", 0, level] = (trust[min(level, len(trust) - 1)], 0)
    out, left = [], set(after)
    while left:
        free = [task for task in left if not any(other in left for other in after[task])]
        task = min(free, key=lambda task: (when[task], task))
        out.append(task)
        left.remove(task)
    return out


def kernel(
    n, mp, width, levels_n, ids_ref, grad_ref, w_ref, master_hbm, m1_hbm, m2_hbm,
    out_ref, new_master_ref, new_first_ref, new_second_ref,
    mine, raw, temp, peak, kept, codes_out, codes_in, scales_out, scales_in, held, held_scale,
    update, sums, member, ratio, tiles, state, units,
    mine_sem, w_sem, own_sem, raw_send, raw_recv, rs_send, rs_recv, ag_send, ag_recv, t_send, t_recv,
):
    me = lax.axis_index("dp")
    bits = [(me // 2**i) % 2 for i in range(n)]
    replicas = 2**n
    _, rows, cols = state.shape
    master_ref, m1_ref, m2_ref = (state.at[i] for i in range(3))
    chunks = cols // width
    lane_groups = width // LANES
    orders = kernel_orders(n, chunks)

    def span(k):
        return pl.ds(k * width, width)

    def partner(flips):
        return sum(2**i * (1 - bits[i] if flips >> i & 1 else bits[i]) for i in range(n))

    low = min(n, 3)
    levels = [[{"dp": partner(f)} for f in range(1, 2**low)]]
    if n > low:
        levels.append([{"dp": partner(f << low)} for f in range(1, 2 ** (n - low))])
    if mp > 1:
        mine_mp = lax.axis_index("mp")
        places = mp.bit_length() - 1
        mp_bits = [(mine_mp // 2**i) % 2 for i in range(places)]
        levels.append([
            {"mp": sum(2**i * (1 - mp_bits[i] if f >> i & 1 else mp_bits[i]) for i in range(places))}
            for f in range(1, mp)
        ])

    w_copy = pltpu.make_async_copy(w_ref, out_ref, w_sem)
    own_copies = [
        pltpu.make_async_copy(src, state.at[i], own_sem) for i, src in enumerate([master_hbm, m1_hbm, m2_hbm])
    ]
    mine_copies = [
        pltpu.make_async_copy(grad_ref.at[:, bits[0], :, span(k)], mine.at[k], mine_sem)
        for k in range(chunks)
    ]
    for copy in mine_copies:
        copy.start()

    barrier = pltpu.get_barrier_semaphore()
    greeted = [target for level in levels for target in level]
    for target in greeted:
        pl.semaphore_signal(barrier, inc=1, device_id=target, device_id_type=MESH)
    pl.semaphore_wait(barrier, len(greeted))

    def finish(ref, sem):
        pltpu.make_async_copy(ref, ref, sem).wait()

    def finish_coded(slots, scales, sem):
        row = LANES * 4
        count = (slots * rows * width * 2 + scales * row) // row
        finish(units.at[pl.ds(0, count)], sem)

    def send(src, dst, send_sem, recv_sem, target):
        copy = pltpu.make_async_remote_copy(
            src_ref=src, dst_ref=dst, send_sem=send_sem, recv_sem=recv_sem,
            device_id=target, device_id_type=MESH,
        )
        copy.start()

    for k in range(chunks):
        send(
            grad_ref.at[:, 1 - bits[0], :, span(k)], raw.at[k], raw_send, raw_recv.at[k], {"dp": partner(1)}
        )
    for copy in own_copies:
        copy.start()
    w_copy.start()

    lane = lax.broadcasted_iota(I32, (1, LANES), 1)

    @pl.loop(0, replicas * rows, unroll=8)
    def _(r):
        member[pl.ds(r, 1), :] = jnp.where(lane == ids_ref[r], 1.0, 0.0).astype(F32)

    sums[...] = jnp.zeros_like(sums)
    correct_one = 1.0 - beta_one**step_count
    correct_two = 1.0 - beta_two**step_count

    def lanes_of(g):
        return pl.ds(g * LANES, LANES)

    def largest(values, so_far):
        for g in range(lane_groups):
            part = jnp.abs(values[:, g * LANES:(g + 1) * LANES])
            for h in range(rows // 8):
                so_far = jnp.maximum(so_far, part[h * 8:(h + 1) * 8])
        return so_far

    def scale_of(most):
        top = jnp.maximum(jnp.max(most, axis=0, keepdims=True), TINY)
        return top * (1.0 / TOP), TOP / top

    def code(value):
        return jnp.round(value).astype(I32).astype(I16)

    def wide(row):
        return jnp.concatenate([row] * lane_groups, axis=1)

    def label_of(order, flags):
        label = [None] * n
        for i, flag in enumerate(flags):
            label[order[n - 1 - i]] = flipped(bits[order[n - 1 - i]], flag)
        for b in range(n):
            if label[b] is None:
                label[b] = bits[b]
        return label

    def both(k, flags):
        rest = sum(2 ** (b - 1) * bit for b, bit in enumerate(label_of(orders[k], flags)) if b)
        return mine[k, rest].astype(F32) + raw[k, rest].astype(F32)

    def reduce(k, s):
        order = orders[k]
        if s == 0:
            if k == first_taken:
                finish(mine, mine_sem)
            finish(raw.at[k], raw_recv.at[k])
        else:
            finish_coded(2 ** (n - 1 - s), 1, rs_recv.at[k, s - 1])
            scale_in = wide(scales_in[s - 1][k])

        def total(flags):
            if s == 0:
                return both(k, flags)
            d = slot(flags)
            got = codes_in[s - 1][k, d].astype(F32) * scale_in
            return (both(k, flags) if s == 1 else kept[k, d]) + got

        if s < n - 1:
            half = 2 ** (n - 2 - s)
            peak[...] = jnp.zeros_like(peak)

            def add(flags):
                value = total(flags)
                temp[slot(flags[:-1])] = value
                peak[...] = largest(value, peak[...])

            over_slots(half, half, add)
            scale, inverse = scale_of(peak[...])
            scales_out[s][k] = scale
            spread = wide(inverse)

            def encode(flags):
                d = slot(flags)
                codes_out[s][k, d] = code(temp[d] * spread)

            over_slots(0, half, encode)
            target = {"dp": partner(1 << order[s + 1])}
            send(codes_out[s].at[k], codes_in[s].at[k], rs_send.at[s, 0], rs_recv.at[k, s], target)
            send(scales_out[s].at[k], scales_in[s].at[k], rs_send.at[s, 1], rs_recv.at[k, s], target)
            if s:

                def keep(flags):
                    kept[k, slot(flags)] = total(flags)

                over_slots(0, half, keep)
            return
        if k == first_done:
            finish(state, own_sem)
        grad_mean = total([]) / replicas
        master = master_ref[:, span(k)]
        new_first = beta_one * m1_ref[:, span(k)] + (1.0 - beta_one) * grad_mean
        new_second = beta_two * m2_ref[:, span(k)] + (1.0 - beta_two) * grad_mean * grad_mean
        change = (
            new_first / correct_one / (jnp.sqrt(new_second / correct_two) + adam_eps)
            + weight_decay * master
        )
        scale, inverse = scale_of(largest(change, jnp.zeros((8, LANES), F32)))
        held_scale[k, 0] = scale
        held[k, 0] = code(change * wide(inverse))
        pass_on(k, -1)
        update[:, span(k)] = change
        new_first_ref[:, span(k)] = new_first
        new_second_ref[:, span(k)] = new_second
        for i, value in enumerate((master, change)):
            square = value * value
            sums[i] += sum(square[:, g * LANES:(g + 1) * LANES] for g in range(lane_groups))

    def gather(k, s, piece):
        target = {"dp": partner(1 << orders[k][n - 1 - s])}
        count = max(2 ** (s - 1), 1)
        first = count if s and piece else 0
        here, there = pl.ds(first, count), pl.ds(first + 2**s, count)
        send(held.at[k, here], held.at[k, there], ag_send.at[s, 0], ag_recv.at[k, s], target)
        send(held_scale.at[k, here], held_scale.at[k, there], ag_send.at[s, 1], ag_recv.at[k, s], target)

    def pass_on(k, s):
        if s + 1 < n:
            gather(k, s + 1, 1)
        if s + 2 < n:
            gather(k, s + 2, 0)

    def expand(k, s):
        finish_coded(2**s, 2**s, ag_recv.at[k, s])
        pass_on(k, s)

    trust_state = {}

    def trust_send(level):
        slots = tiles[level]
        slots[0] = trust_state["sums"]
        for f, target in enumerate(levels[level], 1):
            send(slots.at[0], slots.at[f], t_send.at[level], t_recv.at[level], target)

    def trust_start():
        own = member[pl.ds(pl.multiple_of(me * rows, rows), rows), :]
        w_part = jnp.sum(own * jnp.sum(sums[0], axis=1, keepdims=True), axis=0, keepdims=True)
        u_part = jnp.sum(own * jnp.sum(sums[1], axis=1, keepdims=True), axis=0, keepdims=True)
        sub = lax.broadcasted_iota(I32, (8, LANES), 0)
        trust_state["sums"] = jnp.where(sub == 0, w_part, u_part)
        trust_send(0)

    def trust_next(level):
        total = trust_state["sums"]
        others = len(levels[level])
        finish(tiles[level].at[pl.ds(1, others)], t_recv.at[level])
        for f in range(1, others + 1):
            total = total + tiles[level][f]
        trust_state["sums"] = total
        if level + 1 < len(levels):
            trust_send(level + 1)
            return
        trust = jnp.sqrt(total[0:1] / (total[1:2] + 1e-06))

        @pl.loop(0, replicas, unroll=4)
        def _(d):
            at = pl.ds(pl.multiple_of(d * rows, rows), rows)
            row_ratio = jnp.sum(member[at, :] * trust, axis=1, keepdims=True)
            ratio[at, :] = jnp.broadcast_to(-learn_rate * row_ratio, (rows, LANES))

    def own_master():
        at = pl.ds(pl.multiple_of(me * rows, rows), rows)
        down = ratio[at, :]
        for g in range(cols // LANES):
            new_master_ref[:, lanes_of(g)] = master_ref[:, lanes_of(g)] + down * update[:, lanes_of(g)]

    def apply(k):
        def one(flags):
            d = slot(flags)
            owner = sum(2**b * bit for b, bit in enumerate(label_of(orders[k], flags)))
            at = pl.ds(pl.multiple_of(owner * rows, rows), rows)
            factor = ratio[at, :] * held_scale[k, d]
            delta = (held[k, d].astype(F32) * wide(factor)).astype(BF16)
            out_ref[owner, :, span(k)] = (
                out_ref[owner, :, span(k)].astype(F32) + delta.astype(F32)
            ).astype(BF16)

        over_slots(0, replicas, one)

    order = schedule(n, chunks, len(levels))
    first_taken = order[0][1]
    first_done = next(k for what, k, s in order if what == "R" and s == n - 1)
    for what, k, s in order:
        if what == "R":
            reduce(k, s)
        elif what == "A":
            expand(k, s)
        elif what == "P":
            apply(k)
        elif s == 0:
            trust_start()
        else:
            trust_next(s - 1)
            if s == len(levels):
                own_master()
                w_copy.wait()
    finish(raw, raw_send)
    for s in range(n - 1):
        finish(codes_out[s], rs_send.at[s, 0])
        finish(scales_out[s], rs_send.at[s, 1])
    for s in range(n):
        finish(held.at[:, pl.ds(0, 2**s)], ag_send.at[s, 0])
        finish(held_scale.at[:, pl.ds(0, 2**s)], ag_send.at[s, 1])
    for i, slots in enumerate(tiles):
        finish(slots.at[pl.ds(1, len(levels[i]))], t_send.at[i])


def put_out(a_ref, b_ref, c_ref, d_ref, a_out, b_out, c_out, d_out, sems):
    pairs = [(a_ref, a_out), (b_ref, b_out), (c_ref, c_out), (d_ref, d_out)]
    copies = [pltpu.make_async_copy(src, dst, sems.at[i]) for i, (src, dst) in enumerate(pairs)]
    for copy in copies:
        copy.start()
    for copy in copies:
        copy.wait()


def solution(mesh):
    replicas, mp = mesh.shape["dp"], mesh.shape["mp"]
    n = replicas.bit_length() - 1

    def on_device(gradients, weights, master, moment_one, moment_two, group_ids):
        rows_all, cols = weights.shape
        rows = master.shape[0]
        width = WIDTH if cols % WIDTH == 0 else LANES
        chunks = cols // width
        low = min(n, 3)
        counts = [2**low] + ([2 ** (n - low)] if n > low else []) + ([mp] if mp > 1 else [])
        anywhere = pl.BlockSpec(memory_space=pl.ANY)
        vmem = pl.BlockSpec(memory_space=pltpu.VMEM)
        own = pltpu.VMEM((rows, cols), F32)
        dma = pltpu.SemaphoreType.DMA
        halves = [2 ** (n - 2 - s) for s in range(n - 1)]
        codes = [pltpu.VMEM((chunks, half, rows, width), I16) for half in halves]
        scales = [pltpu.VMEM((chunks, 1, LANES), F32) for _ in halves]
        new_weights, new_master, new_first, new_second = pl.pallas_call(
            functools.partial(kernel, n, mp, width, len(counts)),
            out_shape=(pltpu.VMEM((replicas, rows, cols), BF16), own, own, own),
            in_specs=[pl.BlockSpec(memory_space=pltpu.SMEM)] + [anywhere] * 5,
            out_specs=(vmem, vmem, vmem, vmem),
            scratch_shapes=[
                pltpu.VMEM((chunks, replicas // 2, rows, width), BF16),
                pltpu.VMEM((chunks, replicas // 2, rows, width), BF16),
                pltpu.VMEM((replicas // 4, rows, width), F32),
                pltpu.VMEM((8, LANES), F32),
                pltpu.VMEM((chunks, max(replicas // 8, 1), rows, width), F32),
                codes, codes, scales, scales,
                pltpu.VMEM((chunks, replicas, rows, width), I16),
                pltpu.VMEM((chunks, replicas, 1, LANES), F32),
                pltpu.VMEM((rows, cols), F32),
                pltpu.VMEM((2, rows, LANES), F32),
                pltpu.VMEM((rows_all, LANES), F32),
                pltpu.VMEM((rows_all, LANES), F32),
                [pltpu.VMEM((c, 8, LANES), F32) for c in counts],
                pltpu.VMEM((3, rows, cols), F32),
                pltpu.VMEM((replicas // 2 * (rows * width // (2 * LANES) + 1), 1, LANES), F32),
                dma, dma, dma,
                dma, dma((chunks,)),
                dma((n - 1, 2)), dma((chunks, n - 1)),
                dma((n, 2)), dma((chunks, n)),
                dma((len(counts),)), dma((len(counts),)),
            ],
            compiler_params=pltpu.CompilerParams(
                collective_id=0, has_side_effects=True, vmem_limit_bytes=52 * 2**20
            ),
        )(
            group_ids,
            gradients.reshape(replicas // 2, 2, rows, cols),
            weights.reshape(replicas, rows, cols),
            master, moment_one, moment_two,
        )
        new_weights, new_master, new_first, new_second = pl.pallas_call(
            put_out,
            out_shape=(
                jax.ShapeDtypeStruct((replicas, rows, cols), BF16),
                *[jax.ShapeDtypeStruct((rows, cols), F32)] * 3,
            ),
            in_specs=[vmem] * 4,
            out_specs=(anywhere,) * 4,
            scratch_shapes=[dma((4,))],
            compiler_params=pltpu.CompilerParams(vmem_limit_bytes=2**20),
        )(new_weights, new_master, new_first, new_second)
        return new_weights.reshape(rows_all, cols), new_master, new_first, new_second

    return jax.shard_map(
        on_device,
        mesh=mesh,
        in_specs=(P("dp", None, "mp"), P(None, "mp"), P("dp", "mp"), P("dp", "mp"), P("dp", "mp"), P()),
        out_specs=(P(None, "mp"), P("dp", "mp"), P("dp", "mp"), P("dp", "mp")),
        check_vma=False,
    )
```

```python
import functools

import jax
import jax.numpy as jnp
from jax import lax
from jax.experimental import pallas as pl
from jax.experimental.pallas import tpu as pltpu
from jax.sharding import PartitionSpec as P

beta_one = 0.9
beta_two = 0.999
adam_eps = 1e-06
weight_decay = 0.01
learn_rate = 0.04
step_count = 100

MESH = pl.DeviceIdType.MESH
F32, BF16, I16, I32 = jnp.float32, jnp.bfloat16, jnp.int16, jnp.int32
WIDTH = 512
LANES = 128
STATIC = 8
STAGE_DUE = [0.00, 3.47, 6.19, 9.36, 13.72, 17.22, 21.30, 25.04, 29.23, 40.00]
STAGE_PACE = [2.37, 2.55, 2.91, 2.81, 2.56, 2.76, 2.48, 2.69, 4.82, 4.12]
TRUST_DUE = [26.48, 30.77, 35.67]
PUT_DUE = (37.46, 0.22)
TOP = 32700.0
TINY = 1e-30


def flipped(bit, flag):
    if isinstance(flag, int):
        return 1 - bit if flag else bit
    return bit + flag - 2 * bit * flag


def over_slots(first, count, step):
    fixed = min(count, STATIC)
    places = count.bit_length() - 1
    low = fixed.bit_length() - 1

    def run(high):
        if len(high) < places - low:

            @pl.loop(0, 2)
            def _(bit):
                run([bit] + high)
            return
        for i in range(fixed):
            step([i >> p & 1 for p in range(low)] + high + ([1] if first else []))

    run([])


def slot(flags):
    return sum(2**p * flag for p, flag in enumerate(flags))


def kernel_orders(n, chunks):
    orders = []
    for k in range(chunks):
        order = list(range(n))
        if n > 3:
            order[1:4] = [2, 3, 1] if k % 2 else [1, 3, 2]
        orders.append(order)
    return orders


def schedule(n, chunks, levels):
    if len(STAGE_DUE) == 2 * n:
        due, pace, trust, put = STAGE_DUE, STAGE_PACE, TRUST_DUE, PUT_DUE
    else:
        due, pace = [2.0 * s for s in range(2 * n)], [1.0] * (2 * n)
        trust, put = [due[-1]] * (levels + 1), (due[-1], 1.0)
    after, when = {}, {}
    for k in range(chunks):
        for s in range(2 * n):
            task = ("R", k, s) if s < n else ("A", k, s - n)
            after[task] = [last] if s else []
            when[task] = (due[s] + pace[s] * (k // 2), k)
            last = task
        after["P", k, 0] = [last, ("T", 0, levels)]
        when["P", k, 0] = (put[0] + put[1] * (k // 2), k)
    for level in range(levels + 1):
        after["T", 0, level] = [("T", 0, level - 1)] if level else [("R", k, n - 1) for k in range(chunks)]
        when["T", 0, level] = (trust[min(level, len(trust) - 1)], 0)
    out, left = [], set(after)
    while left:
        free = [task for task in left if not any(other in left for other in after[task])]
        task = min(free, key=lambda task: (when[task], task))
        out.append(task)
        left.remove(task)
    return out


def kernel(
    n, mp, width, levels_n, ids_hbm, grad_ref, w_ref, master_hbm, m1_hbm, m2_hbm,
    out_ref, new_master_ref, new_first_ref, new_second_ref,
    mine, raw, temp, peak, kept, codes_out, codes_in, scales_out, scales_in, held, held_scale,
    update, sums, member, ratio, tiles, state, units, ids_ref,
    mine_sem, w_sem, own_sem, ids_sem, raw_send, raw_recv, rs_send, rs_recv, ag_send, ag_recv, t_send, t_recv,
):
    me = lax.axis_index("dp")
    bits = [(me // 2**i) % 2 for i in range(n)]
    replicas = 2**n
    _, rows, cols = state.shape
    master_ref, m1_ref, m2_ref = (state.at[i] for i in range(3))
    chunks = cols // width
    lane_groups = width // LANES
    orders = kernel_orders(n, chunks)

    def span(k):
        return pl.ds(k * width, width)

    def partner(flips):
        return sum(2**i * (1 - bits[i] if flips >> i & 1 else bits[i]) for i in range(n))

    low = min(n, 3)
    levels = [[{"dp": partner(f)} for f in range(1, 2**low)]]
    if n > low:
        levels.append([{"dp": partner(f << low)} for f in range(1, 2 ** (n - low))])
    if mp > 1:
        mine_mp = lax.axis_index("mp")
        places = mp.bit_length() - 1
        mp_bits = [(mine_mp // 2**i) % 2 for i in range(places)]
        levels.append([
            {"mp": sum(2**i * (1 - mp_bits[i] if f >> i & 1 else mp_bits[i]) for i in range(places))}
            for f in range(1, mp)
        ])

    w_copy = pltpu.make_async_copy(w_ref, out_ref, w_sem)
    own_copies = [
        pltpu.make_async_copy(src, state.at[i], own_sem) for i, src in enumerate([master_hbm, m1_hbm, m2_hbm])
    ]
    mine_copies = [
        pltpu.make_async_copy(grad_ref.at[:, bits[0], :, span(k)], mine.at[k], mine_sem)
        for k in range(chunks)
    ]

    barrier = pltpu.get_barrier_semaphore()
    greeted = [target for level in levels for target in level]
    for target in greeted:
        pl.semaphore_signal(barrier, inc=1, device_id=target, device_id_type=MESH)
    ids_copy = pltpu.make_async_copy(ids_hbm, ids_ref, ids_sem)
    ids_copy.start()
    for copy in mine_copies:
        copy.start()
    pl.semaphore_wait(barrier, len(greeted))

    def finish(ref, sem):
        pltpu.make_async_copy(ref, ref, sem).wait()

    def finish_coded(slots, scales, sem):
        row = LANES * 4
        count = (slots * rows * width * 2 + scales * row) // row
        finish(units.at[pl.ds(0, count)], sem)

    def send(src, dst, send_sem, recv_sem, target):
        copy = pltpu.make_async_remote_copy(
            src_ref=src, dst_ref=dst, send_sem=send_sem, recv_sem=recv_sem,
            device_id=target, device_id_type=MESH,
        )
        copy.start()

    for k in range(chunks):
        send(
            grad_ref.at[:, 1 - bits[0], :, span(k)], raw.at[k], raw_send, raw_recv.at[k], {"dp": partner(1)}
        )
    for copy in own_copies:
        copy.start()
    w_copy.start()

    ids_copy.wait()
    lane = lax.broadcasted_iota(I32, (1, LANES), 1)

    @pl.loop(0, replicas * rows, unroll=8)
    def _(r):
        member[pl.ds(r, 1), :] = jnp.where(lane == ids_ref[r], 1.0, 0.0).astype(F32)

    sums[...] = jnp.zeros_like(sums)
    correct_one = 1.0 - beta_one**step_count
    correct_two = 1.0 - beta_two**step_count

    def lanes_of(g):
        return pl.ds(g * LANES, LANES)

    def largest(values, so_far):
        for g in range(lane_groups):
            part = jnp.abs(values[:, g * LANES:(g + 1) * LANES])
            for h in range(rows // 8):
                so_far = jnp.maximum(so_far, part[h * 8:(h + 1) * 8])
        return so_far

    def scale_of(most):
        top = jnp.maximum(jnp.max(most, axis=0, keepdims=True), TINY)
        return top * (1.0 / TOP), TOP / top

    def code(value):
        return jnp.round(value).astype(I32).astype(I16)

    def wide(row):
        return jnp.concatenate([row] * lane_groups, axis=1)

    def label_of(order, flags):
        label = [None] * n
        for i, flag in enumerate(flags):
            label[order[n - 1 - i]] = flipped(bits[order[n - 1 - i]], flag)
        for b in range(n):
            if label[b] is None:
                label[b] = bits[b]
        return label

    def both(k, flags):
        rest = sum(2 ** (b - 1) * bit for b, bit in enumerate(label_of(orders[k], flags)) if b)
        return mine[k, rest].astype(F32) + raw[k, rest].astype(F32)

    def reduce(k, s):
        order = orders[k]
        if s == 0:
            if k == first_taken:
                finish(mine, mine_sem)
            finish(raw.at[k], raw_recv.at[k])
        else:
            finish_coded(2 ** (n - 1 - s), 1, rs_recv.at[k, s - 1])
            scale_in = wide(scales_in[s - 1][k])

        def total(flags):
            if s == 0:
                return both(k, flags)
            d = slot(flags)
            got = codes_in[s - 1][k, d].astype(F32) * scale_in
            return (both(k, flags) if s == 1 else kept[k, d]) + got

        if s < n - 1:
            half = 2 ** (n - 2 - s)
            peak[...] = jnp.zeros_like(peak)

            def add(flags):
                value = total(flags)
                temp[slot(flags[:-1])] = value
                peak[...] = largest(value, peak[...])

            over_slots(half, half, add)
            scale, inverse = scale_of(peak[...])
            scales_out[s][k] = scale
            spread = wide(inverse)

            def encode(flags):
                d = slot(flags)
                codes_out[s][k, d] = code(temp[d] * spread)

            over_slots(0, half, encode)
            target = {"dp": partner(1 << order[s + 1])}
            send(codes_out[s].at[k], codes_in[s].at[k], rs_send.at[s, 0], rs_recv.at[k, s], target)
            send(scales_out[s].at[k], scales_in[s].at[k], rs_send.at[s, 1], rs_recv.at[k, s], target)
            if s:

                def keep(flags):
                    kept[k, slot(flags)] = total(flags)

                over_slots(0, half, keep)
            return
        if k == first_done:
            finish(state, own_sem)
        grad_mean = total([]) / replicas
        master = master_ref[:, span(k)]
        new_first = beta_one * m1_ref[:, span(k)] + (1.0 - beta_one) * grad_mean
        new_second = beta_two * m2_ref[:, span(k)] + (1.0 - beta_two) * grad_mean * grad_mean
        change = (
            new_first / correct_one / (jnp.sqrt(new_second / correct_two) + adam_eps)
            + weight_decay * master
        )
        scale, inverse = scale_of(largest(change, jnp.zeros((8, LANES), F32)))
        held_scale[k, 0] = scale
        held[k, 0] = code(change * wide(inverse))
        pass_on(k, -1)
        update[:, span(k)] = change
        new_first_ref[:, span(k)] = new_first
        new_second_ref[:, span(k)] = new_second
        for i, value in enumerate((master, change)):
            square = value * value
            sums[i] += sum(square[:, g * LANES:(g + 1) * LANES] for g in range(lane_groups))

    def gather(k, s, piece):
        target = {"dp": partner(1 << orders[k][n - 1 - s])}
        count = max(2 ** (s - 1), 1)
        first = count if s and piece else 0
        here, there = pl.ds(first, count), pl.ds(first + 2**s, count)
        send(held.at[k, here], held.at[k, there], ag_send.at[s, 0], ag_recv.at[k, s], target)
        if piece:
            here, there = pl.ds(0, 2**s), pl.ds(2**s, 2**s)
            send(held_scale.at[k, here], held_scale.at[k, there], ag_send.at[s, 1], ag_recv.at[k, s], target)

    def pass_on(k, s):
        if s + 1 < n:
            gather(k, s + 1, 1)
        if s + 2 < n:
            gather(k, s + 2, 0)

    def expand(k, s):
        finish_coded(2**s, 2**s, ag_recv.at[k, s])
        pass_on(k, s)

    trust_state = {}

    def trust_send(level):
        slots = tiles[level]
        slots[0] = trust_state["sums"]
        for f, target in enumerate(levels[level], 1):
            send(slots.at[0], slots.at[f], t_send.at[level], t_recv.at[level], target)

    def trust_start():
        own = member[pl.ds(pl.multiple_of(me * rows, rows), rows), :]
        w_part = jnp.sum(own * jnp.sum(sums[0], axis=1, keepdims=True), axis=0, keepdims=True)
        u_part = jnp.sum(own * jnp.sum(sums[1], axis=1, keepdims=True), axis=0, keepdims=True)
        sub = lax.broadcasted_iota(I32, (8, LANES), 0)
        trust_state["sums"] = jnp.where(sub == 0, w_part, u_part)
        trust_send(0)

    def trust_next(level):
        total = trust_state["sums"]
        others = len(levels[level])
        finish(tiles[level].at[pl.ds(1, others)], t_recv.at[level])
        for f in range(1, others + 1):
            total = total + tiles[level][f]
        trust_state["sums"] = total
        if level + 1 < len(levels):
            trust_send(level + 1)
            return
        trust = jnp.sqrt(total[0:1] / (total[1:2] + 1e-06))

        @pl.loop(0, replicas, unroll=4)
        def _(d):
            at = pl.ds(pl.multiple_of(d * rows, rows), rows)
            row_ratio = jnp.sum(member[at, :] * trust, axis=1, keepdims=True)
            ratio[at, :] = jnp.broadcast_to(-learn_rate * row_ratio, (rows, LANES))

    def own_master():
        at = pl.ds(pl.multiple_of(me * rows, rows), rows)
        down = ratio[at, :]
        for g in range(cols // LANES):
            new_master_ref[:, lanes_of(g)] = master_ref[:, lanes_of(g)] + down * update[:, lanes_of(g)]

    def apply(k):
        def one(flags):
            d = slot(flags)
            owner = sum(2**b * bit for b, bit in enumerate(label_of(orders[k], flags)))
            at = pl.ds(pl.multiple_of(owner * rows, rows), rows)
            factor = ratio[at, :] * held_scale[k, d]
            delta = (held[k, d].astype(F32) * wide(factor)).astype(BF16)
            out_ref[owner, :, span(k)] = (
                out_ref[owner, :, span(k)].astype(F32) + delta.astype(F32)
            ).astype(BF16)

        over_slots(0, replicas, one)

    order = schedule(n, chunks, len(levels))
    first_taken = order[0][1]
    first_done = next(k for what, k, s in order if what == "R" and s == n - 1)
    for what, k, s in order:
        if what == "R":
            reduce(k, s)
        elif what == "A":
            expand(k, s)
        elif what == "P":
            apply(k)
        elif s == 0:
            trust_start()
        else:
            trust_next(s - 1)
            if s == len(levels):
                own_master()
                w_copy.wait()
    finish(raw, raw_send)
    for s in range(n - 1):
        finish(codes_out[s], rs_send.at[s, 0])
        finish(scales_out[s], rs_send.at[s, 1])
    for s in range(n):
        finish(held.at[:, pl.ds(0, 2**s)], ag_send.at[s, 0])
        finish(held_scale.at[:, pl.ds(0, 2**s)], ag_send.at[s, 1])
    for i, slots in enumerate(tiles):
        finish(slots.at[pl.ds(1, len(levels[i]))], t_send.at[i])


def put_out(a_ref, b_ref, c_ref, d_ref, a_out, b_out, c_out, d_out, sems):
    pairs = [(a_ref, a_out), (b_ref, b_out), (c_ref, c_out), (d_ref, d_out)]
    copies = [pltpu.make_async_copy(src, dst, sems.at[i]) for i, (src, dst) in enumerate(pairs)]
    for copy in copies:
        copy.start()
    for copy in copies:
        copy.wait()


def solution(mesh):
    replicas, mp = mesh.shape["dp"], mesh.shape["mp"]
    n = replicas.bit_length() - 1

    def on_device(gradients, weights, master, moment_one, moment_two, group_ids):
        rows_all, cols = weights.shape
        rows = master.shape[0]
        width = WIDTH if cols % WIDTH == 0 else LANES
        chunks = cols // width
        low = min(n, 3)
        counts = [2**low] + ([2 ** (n - low)] if n > low else []) + ([mp] if mp > 1 else [])
        anywhere = pl.BlockSpec(memory_space=pl.ANY)
        vmem = pl.BlockSpec(memory_space=pltpu.VMEM)
        own = pltpu.VMEM((rows, cols), F32)
        dma = pltpu.SemaphoreType.DMA
        halves = [2 ** (n - 2 - s) for s in range(n - 1)]
        codes = [pltpu.VMEM((chunks, half, rows, width), I16) for half in halves]
        scales = [pltpu.VMEM((chunks, 1, LANES), F32) for _ in halves]
        new_weights, new_master, new_first, new_second = pl.pallas_call(
            functools.partial(kernel, n, mp, width, len(counts)),
            out_shape=(pltpu.VMEM((replicas, rows, cols), BF16), own, own, own),
            in_specs=[anywhere] * 6,
            out_specs=(vmem, vmem, vmem, vmem),
            scratch_shapes=[
                pltpu.VMEM((chunks, replicas // 2, rows, width), BF16),
                pltpu.VMEM((chunks, replicas // 2, rows, width), BF16),
                pltpu.VMEM((replicas // 4, rows, width), F32),
                pltpu.VMEM((8, LANES), F32),
                pltpu.VMEM((chunks, max(replicas // 8, 1), rows, width), F32),
                codes, codes, scales, scales,
                pltpu.VMEM((chunks, replicas, rows, width), I16),
                pltpu.VMEM((chunks, replicas, 1, LANES), F32),
                pltpu.VMEM((rows, cols), F32),
                pltpu.VMEM((2, rows, LANES), F32),
                pltpu.VMEM((rows_all, LANES), F32),
                pltpu.VMEM((rows_all, LANES), F32),
                [pltpu.VMEM((c, 8, LANES), F32) for c in counts],
                pltpu.VMEM((3, rows, cols), F32),
                pltpu.VMEM((replicas // 2 * (rows * width // (2 * LANES) + 1), 1, LANES), F32),
                pltpu.SMEM((rows_all,), I32),
                dma, dma, dma, dma,
                dma, dma((chunks,)),
                dma((n - 1, 2)), dma((chunks, n - 1)),
                dma((n, 2)), dma((chunks, n)),
                dma((len(counts),)), dma((len(counts),)),
            ],
            compiler_params=pltpu.CompilerParams(
                collective_id=0, has_side_effects=True, vmem_limit_bytes=52 * 2**20
            ),
        )(
            group_ids,
            gradients.reshape(replicas // 2, 2, rows, cols),
            weights.reshape(replicas, rows, cols),
            master, moment_one, moment_two,
        )
        new_weights, new_master, new_first, new_second = pl.pallas_call(
            put_out,
            out_shape=(
                jax.ShapeDtypeStruct((replicas, rows, cols), BF16),
                *[jax.ShapeDtypeStruct((rows, cols), F32)] * 3,
            ),
            in_specs=[vmem] * 4,
            out_specs=(anywhere,) * 4,
            scratch_shapes=[dma((4,))],
            compiler_params=pltpu.CompilerParams(vmem_limit_bytes=2**20),
        )(new_weights, new_master, new_first, new_second)
        return new_weights.reshape(rows_all, cols), new_master, new_first, new_second

    return jax.shard_map(
        on_device,
        mesh=mesh,
        in_specs=(P("dp", None, "mp"), P(None, "mp"), P("dp", "mp"), P("dp", "mp"), P("dp", "mp"), P()),
        out_specs=(P(None, "mp"), P("dp", "mp"), P("dp", "mp"), P("dp", "mp")),
        check_vma=False,
    )
```

```python
import functools

import jax
import jax.numpy as jnp
from jax import lax
from jax.experimental import pallas as pl
from jax.experimental.pallas import tpu as pltpu
from jax.sharding import PartitionSpec as P

beta_one = 0.9
beta_two = 0.999
adam_eps = 1e-06
weight_decay = 0.01
learn_rate = 0.04
step_count = 100

MESH = pl.DeviceIdType.MESH
F32, BF16, I16, I32 = jnp.float32, jnp.bfloat16, jnp.int16, jnp.int32
WIDTH = 512
LANES = 128
STATIC = 8
PARTS = 8
STAGE_DUE = [0.00, 3.47, 6.19, 9.36, 13.72, 17.22, 21.30, 25.04, 29.23, 40.00]
STAGE_PACE = [2.37, 2.55, 2.91, 2.81, 2.56, 2.76, 2.48, 2.69, 4.82, 4.12]
TRUST_DUE = [26.48, 30.77, 35.67]
PUT_DUE = (37.46, 0.22)
TOP = 32700.0
TINY = 1e-30


def flipped(bit, flag):
    if isinstance(flag, int):
        return 1 - bit if flag else bit
    return bit + flag - 2 * bit * flag


def over_slots(first, count, step):
    fixed = min(count, STATIC)
    places = count.bit_length() - 1
    low = fixed.bit_length() - 1

    def run(high):
        if len(high) < places - low:

            @pl.loop(0, 2)
            def _(bit):
                run([bit] + high)
            return
        for i in range(fixed):
            step([i >> p & 1 for p in range(low)] + high + ([1] if first else []))

    run([])


def slot(flags):
    return sum(2**p * flag for p, flag in enumerate(flags))


def kernel_orders(n, chunks):
    orders = []
    for k in range(chunks):
        order = list(range(n))
        if n > 3:
            order[1:4] = [2, 3, 1] if k % 2 else [1, 3, 2]
        orders.append(order)
    return orders


def schedule(n, chunks, levels):
    if len(STAGE_DUE) == 2 * n:
        due, pace, trust, put = STAGE_DUE, STAGE_PACE, TRUST_DUE, PUT_DUE
    else:
        due, pace = [2.0 * s for s in range(2 * n)], [1.0] * (2 * n)
        trust, put = [due[-1]] * (levels + 1), (due[-1], 1.0)
    after, when = {}, {}
    for k in range(chunks):
        for s in range(2 * n):
            task = ("R", k, s) if s < n else ("A", k, s - n)
            after[task] = [last] if s else []
            when[task] = (due[s] + pace[s] * (k // 2), k)
            last = task
        after["P", k, 0] = [last, ("T", 0, levels)]
        when["P", k, 0] = (put[0] + put[1] * (k // 2), k)
    for level in range(levels + 1):
        after["T", 0, level] = [("T", 0, level - 1)] if level else [("R", k, n - 1) for k in range(chunks)]
        when["T", 0, level] = (trust[min(level, len(trust) - 1)], 0)
    out, left = [], set(after)
    while left:
        free = [task for task in left if not any(other in left for other in after[task])]
        task = min(free, key=lambda task: (when[task], task))
        out.append(task)
        left.remove(task)
    return out


def kernel(
    n, mp, width, levels_n, ids_hbm, grad_ref, w_ref, master_hbm, m1_hbm, m2_hbm,
    out_ref, new_master_ref, new_first_ref, new_second_ref,
    mine, raw, temp, peak, kept, codes_out, codes_in, scales_out, scales_in, held, held_scale,
    update, sums, member, ratio, tiles, state, units, ids_ref,
    mine_sem, w_sem, own_sem, ids_sem, raw_send, raw_recv, rs_send, rs_recv, ag_send, ag_recv, t_send, t_recv,
):
    me = lax.axis_index("dp")
    bits = [(me // 2**i) % 2 for i in range(n)]
    replicas = 2**n
    _, rows, cols = state.shape
    master_ref, m1_ref, m2_ref = (state.at[i] for i in range(3))
    chunks = cols // width
    lane_groups = width // LANES
    orders = kernel_orders(n, chunks)

    def span(k):
        return pl.ds(k * width, width)

    def partner(flips):
        return sum(2**i * (1 - bits[i] if flips >> i & 1 else bits[i]) for i in range(n))

    low = min(n, 3)
    levels = [[{"dp": partner(f)} for f in range(1, 2**low)]]
    if n > low:
        levels.append([{"dp": partner(f << low)} for f in range(1, 2 ** (n - low))])
    if mp > 1:
        mine_mp = lax.axis_index("mp")
        places = mp.bit_length() - 1
        mp_bits = [(mine_mp // 2**i) % 2 for i in range(places)]
        levels.append([
            {"mp": sum(2**i * (1 - mp_bits[i] if f >> i & 1 else mp_bits[i]) for i in range(places))}
            for f in range(1, mp)
        ])

    w_copy = pltpu.make_async_copy(w_ref, out_ref, w_sem)
    own_copies = [
        pltpu.make_async_copy(src, state.at[i], own_sem) for i, src in enumerate([master_hbm, m1_hbm, m2_hbm])
    ]
    mine_copies = [
        pltpu.make_async_copy(grad_ref.at[:, bits[0], :, span(k)], mine.at[k], mine_sem)
        for k in range(chunks)
    ]

    barrier = pltpu.get_barrier_semaphore()
    greeted = [target for level in levels for target in level]
    for target in greeted:
        pl.semaphore_signal(barrier, inc=1, device_id=target, device_id_type=MESH)
    ids_copy = pltpu.make_async_copy(ids_hbm, ids_ref, ids_sem)
    ids_copy.start()
    for copy in mine_copies:
        copy.start()
    pl.semaphore_wait(barrier, len(greeted))

    def finish(ref, sem):
        pltpu.make_async_copy(ref, ref, sem).wait()

    def finish_coded(slots, scales, sem):
        row = LANES * 4
        count = (slots * rows * width * 2 + scales * row) // row
        finish(units.at[pl.ds(0, count)], sem)

    def send(src, dst, send_sem, recv_sem, target):
        copy = pltpu.make_async_remote_copy(
            src_ref=src, dst_ref=dst, send_sem=send_sem, recv_sem=recv_sem,
            device_id=target, device_id_type=MESH,
        )
        copy.start()

    for k in range(chunks):
        send(
            grad_ref.at[:, 1 - bits[0], :, span(k)], raw.at[k], raw_send, raw_recv.at[k], {"dp": partner(1)}
        )
    for copy in own_copies:
        copy.start()
    w_copy.start()

    ids_copy.wait()
    lane = lax.broadcasted_iota(I32, (1, LANES), 1)

    @pl.loop(0, replicas * rows, unroll=8)
    def _(r):
        member[pl.ds(r, 1), :] = jnp.where(lane == ids_ref[r], 1.0, 0.0).astype(F32)

    sums[...] = jnp.zeros_like(sums)
    correct_one = 1.0 - beta_one**step_count
    correct_two = 1.0 - beta_two**step_count

    def lanes_of(g):
        return pl.ds(g * LANES, LANES)

    def largest(values, so_far):
        for g in range(lane_groups):
            part = jnp.abs(values[:, g * LANES:(g + 1) * LANES])
            for h in range(rows // 8):
                so_far = jnp.maximum(so_far, part[h * 8:(h + 1) * 8])
        return so_far

    def scale_of(most):
        top = jnp.maximum(jnp.max(most, axis=0, keepdims=True), TINY)
        return top * (1.0 / TOP), TOP / top

    def code(value):
        return jnp.round(value).astype(I32).astype(I16)

    def wide(row):
        return jnp.concatenate([row] * lane_groups, axis=1)

    def label_of(order, flags):
        label = [None] * n
        for i, flag in enumerate(flags):
            label[order[n - 1 - i]] = flipped(bits[order[n - 1 - i]], flag)
        for b in range(n):
            if label[b] is None:
                label[b] = bits[b]
        return label

    def both(k, flags):
        rest = sum(2 ** (b - 1) * bit for b, bit in enumerate(label_of(orders[k], flags)) if b)
        return mine[k, rest].astype(F32) + raw[k, rest].astype(F32)

    def reduce(k, s):
        order = orders[k]
        if s == 0:
            if k == first_taken:
                finish(mine, mine_sem)
            finish(raw.at[k], raw_recv.at[k])
        else:
            finish_coded(2 ** (n - 1 - s), 1, rs_recv.at[k, s - 1])
            scale_in = wide(scales_in[s - 1][k])

        def total(flags):
            if s == 0:
                return both(k, flags)
            d = slot(flags)
            got = codes_in[s - 1][k, d].astype(F32) * scale_in
            return (both(k, flags) if s == 1 else kept[k, d]) + got

        if s < n - 1:
            half = 2 ** (n - 2 - s)
            peak[...] = jnp.zeros_like(peak)

            def add(flags):
                value = total(flags)
                temp[slot(flags[:-1])] = value
                peak[...] = largest(value, peak[...])

            over_slots(half, half, add)
            scale, inverse = scale_of(peak[...])
            scales_out[s][k] = scale
            spread = wide(inverse)

            def encode(flags):
                d = slot(flags)
                codes_out[s][k, d] = code(temp[d] * spread)

            over_slots(0, half, encode)
            target = {"dp": partner(1 << order[s + 1])}
            send(codes_out[s].at[k], codes_in[s].at[k], rs_send.at[s, 0], rs_recv.at[k, s], target)
            send(scales_out[s].at[k], scales_in[s].at[k], rs_send.at[s, 1], rs_recv.at[k, s], target)
            if s:

                def keep(flags):
                    kept[k, slot(flags)] = total(flags)

                over_slots(0, half, keep)
            return
        if k == first_done:
            finish(state, own_sem)
        grad_mean = total([]) / replicas
        master = master_ref[:, span(k)]
        new_first = beta_one * m1_ref[:, span(k)] + (1.0 - beta_one) * grad_mean
        new_second = beta_two * m2_ref[:, span(k)] + (1.0 - beta_two) * grad_mean * grad_mean
        change = (
            new_first / correct_one / (jnp.sqrt(new_second / correct_two) + adam_eps)
            + weight_decay * master
        )
        scale, inverse = scale_of(largest(change, jnp.zeros((8, LANES), F32)))
        held_scale[k, 0] = scale
        held[k, 0] = code(change * wide(inverse))
        pass_on(k, -1)
        update[:, span(k)] = change
        new_first_ref[:, span(k)] = new_first
        new_second_ref[:, span(k)] = new_second
        for i, value in enumerate((master, change)):
            square = value * value
            sums[i] += sum(square[:, g * LANES:(g + 1) * LANES] for g in range(lane_groups))

    def gather(k, s, piece):
        target = {"dp": partner(1 << orders[k][n - 1 - s])}
        count = max(2 ** (s - 1), 1)
        first = count if s and piece else 0
        here, there = pl.ds(first, count), pl.ds(first + 2**s, count)
        send(held.at[k, here], held.at[k, there], ag_send.at[s, 0], ag_recv.at[k, s], target)
        if piece:
            here, there = pl.ds(0, 2**s), pl.ds(2**s, 2**s)
            send(held_scale.at[k, here], held_scale.at[k, there], ag_send.at[s, 1], ag_recv.at[k, s], target)

    def pass_on(k, s):
        if s + 1 < n:
            gather(k, s + 1, 1)
        if s + 2 < n:
            gather(k, s + 2, 0)

    def expand(k, s):
        finish_coded(2**s, 2**s, ag_recv.at[k, s])
        pass_on(k, s)

    trust_state = {}

    def trust_send(level):
        slots = tiles[level]
        slots[0] = trust_state["sums"]
        for f, target in enumerate(levels[level], 1):
            send(slots.at[0], slots.at[f], t_send.at[level], t_recv.at[level], target)

    def trust_start():
        own = member[pl.ds(pl.multiple_of(me * rows, rows), rows), :]
        w_part = jnp.sum(own * jnp.sum(sums[0], axis=1, keepdims=True), axis=0, keepdims=True)
        u_part = jnp.sum(own * jnp.sum(sums[1], axis=1, keepdims=True), axis=0, keepdims=True)
        sub = lax.broadcasted_iota(I32, (8, LANES), 0)
        trust_state["sums"] = jnp.where(sub == 0, w_part, u_part)
        trust_send(0)

    def trust_next(level):
        total = trust_state["sums"]
        others = len(levels[level])
        finish(tiles[level].at[pl.ds(1, others)], t_recv.at[level])
        for f in range(1, others + 1):
            total = total + tiles[level][f]
        trust_state["sums"] = total
        if level + 1 < len(levels):
            trust_send(level + 1)
            return
        trust = jnp.sqrt(total[0:1] / (total[1:2] + 1e-06))

        @pl.loop(0, replicas, unroll=4)
        def _(d):
            at = pl.ds(pl.multiple_of(d * rows, rows), rows)
            row_ratio = jnp.sum(member[at, :] * trust, axis=1, keepdims=True)
            ratio[at, :] = jnp.broadcast_to(-learn_rate * row_ratio, (rows, LANES))

    def own_master():
        at = pl.ds(pl.multiple_of(me * rows, rows), rows)
        down = ratio[at, :]
        for g in range(cols // LANES):
            new_master_ref[:, lanes_of(g)] = master_ref[:, lanes_of(g)] + down * update[:, lanes_of(g)]

    def apply(k):
        def one(flags):
            d = slot(flags)
            owner = sum(2**b * bit for b, bit in enumerate(label_of(orders[k], flags)))
            at = pl.ds(pl.multiple_of(owner * rows, rows), rows)
            factor = ratio[at, :] * held_scale[k, d]
            delta = (held[k, d].astype(F32) * wide(factor)).astype(BF16)
            out_ref[owner, :, span(k)] = (
                out_ref[owner, :, span(k)].astype(F32) + delta.astype(F32)
            ).astype(BF16)

        over_slots(0, replicas, one)

    order = schedule(n, chunks, len(levels))
    first_taken = order[0][1]
    first_done = next(k for what, k, s in order if what == "R" and s == n - 1)
    for what, k, s in order:
        if what == "R":
            reduce(k, s)
        elif what == "A":
            expand(k, s)
        elif what == "P":
            apply(k)
        elif s == 0:
            trust_start()
        else:
            trust_next(s - 1)
            if s == len(levels):
                own_master()
                w_copy.wait()
    finish(raw, raw_send)
    for s in range(n - 1):
        finish(codes_out[s], rs_send.at[s, 0])
        finish(scales_out[s], rs_send.at[s, 1])
    for s in range(n):
        finish(held.at[:, pl.ds(0, 2**s)], ag_send.at[s, 0])
        finish(held_scale.at[:, pl.ds(0, 2**s)], ag_send.at[s, 1])
    for i, slots in enumerate(tiles):
        finish(slots.at[pl.ds(1, len(levels[i]))], t_send.at[i])


def put_out(a_ref, b_ref, c_ref, d_ref, a_out, b_out, c_out, d_out, sems):
    part = a_ref.shape[0] // PARTS
    pairs = [(a_ref.at[pl.ds(i * part, part)], a_out.at[pl.ds(i * part, part)]) for i in range(PARTS)]
    pairs += [(b_ref, b_out), (c_ref, c_out), (d_ref, d_out)]
    copies = [pltpu.make_async_copy(src, dst, sems.at[i]) for i, (src, dst) in enumerate(pairs)]
    for copy in copies:
        copy.start()
    for copy in copies:
        copy.wait()


def solution(mesh):
    replicas, mp = mesh.shape["dp"], mesh.shape["mp"]
    n = replicas.bit_length() - 1

    def on_device(gradients, weights, master, moment_one, moment_two, group_ids):
        rows_all, cols = weights.shape
        rows = master.shape[0]
        width = WIDTH if cols % WIDTH == 0 else LANES
        chunks = cols // width
        low = min(n, 3)
        counts = [2**low] + ([2 ** (n - low)] if n > low else []) + ([mp] if mp > 1 else [])
        anywhere = pl.BlockSpec(memory_space=pl.ANY)
        vmem = pl.BlockSpec(memory_space=pltpu.VMEM)
        own = pltpu.VMEM((rows, cols), F32)
        dma = pltpu.SemaphoreType.DMA
        halves = [2 ** (n - 2 - s) for s in range(n - 1)]
        codes = [pltpu.VMEM((chunks, half, rows, width), I16) for half in halves]
        scales = [pltpu.VMEM((chunks, 1, LANES), F32) for _ in halves]
        new_weights, new_master, new_first, new_second = pl.pallas_call(
            functools.partial(kernel, n, mp, width, len(counts)),
            out_shape=(pltpu.VMEM((replicas, rows, cols), BF16), own, own, own),
            in_specs=[anywhere] * 6,
            out_specs=(vmem, vmem, vmem, vmem),
            scratch_shapes=[
                pltpu.VMEM((chunks, replicas // 2, rows, width), BF16),
                pltpu.VMEM((chunks, replicas // 2, rows, width), BF16),
                pltpu.VMEM((replicas // 4, rows, width), F32),
                pltpu.VMEM((8, LANES), F32),
                pltpu.VMEM((chunks, max(replicas // 8, 1), rows, width), F32),
                codes, codes, scales, scales,
                pltpu.VMEM((chunks, replicas, rows, width), I16),
                pltpu.VMEM((chunks, replicas, 1, LANES), F32),
                pltpu.VMEM((rows, cols), F32),
                pltpu.VMEM((2, rows, LANES), F32),
                pltpu.VMEM((rows_all, LANES), F32),
                pltpu.VMEM((rows_all, LANES), F32),
                [pltpu.VMEM((c, 8, LANES), F32) for c in counts],
                pltpu.VMEM((3, rows, cols), F32),
                pltpu.VMEM((replicas // 2 * (rows * width // (2 * LANES) + 1), 1, LANES), F32),
                pltpu.SMEM((rows_all,), I32),
                dma, dma, dma, dma,
                dma, dma((chunks,)),
                dma((n - 1, 2)), dma((chunks, n - 1)),
                dma((n, 2)), dma((chunks, n)),
                dma((len(counts),)), dma((len(counts),)),
            ],
            compiler_params=pltpu.CompilerParams(
                collective_id=0, has_side_effects=True, vmem_limit_bytes=52 * 2**20
            ),
        )(
            group_ids,
            gradients.reshape(replicas // 2, 2, rows, cols),
            weights.reshape(replicas, rows, cols),
            master, moment_one, moment_two,
        )
        new_weights, new_master, new_first, new_second = pl.pallas_call(
            put_out,
            out_shape=(
                jax.ShapeDtypeStruct((replicas, rows, cols), BF16),
                *[jax.ShapeDtypeStruct((rows, cols), F32)] * 3,
            ),
            in_specs=[vmem] * 4,
            out_specs=(anywhere,) * 4,
            scratch_shapes=[dma((PARTS + 3,))],
            compiler_params=pltpu.CompilerParams(vmem_limit_bytes=2**20),
        )(new_weights, new_master, new_first, new_second)
        return new_weights.reshape(rows_all, cols), new_master, new_first, new_second

    return jax.shard_map(
        on_device,
        mesh=mesh,
        in_specs=(P("dp", None, "mp"), P(None, "mp"), P("dp", "mp"), P("dp", "mp"), P("dp", "mp"), P()),
        out_specs=(P(None, "mp"), P("dp", "mp"), P("dp", "mp"), P("dp", "mp")),
        check_vma=False,
    )
```
